32 devices in a mesh: lon: 8 (over y, x, core), lat: 4 (over z).
Axes of the slice: x: 2, y: 2, z: 4, core: 2. Of those that a mesh axis runs over, the one named last changes fastest.
Arguments:
- grid_latent: bfloat16 [4, 8, 1024, 512], P('lat', 'lon'), may hold values from -6 to 6
- mesh_latent: bfloat16 [4, 8, 160, 512], P('lat', 'lon'), may hold values from -6 to 6
- edge_geometry: float32 [4, 8, 4, 2048], P('lat', 'lon'), may hold values from -6 to 6
- senders: int32 [4, 8, 2048], P('lat', 'lon'), may hold values from 0 to 1023
- receivers: int32 [4, 8, 2048], P('lat', 'lon'), may hold values from 0 to 1439, as said below
- w_grid: bfloat16 [512, 512], replicated, may hold values from -0.25 to 0.25
- w_mesh: bfloat16 [512, 512], replicated, may hold values from -0.25 to 0.25
- w_edge: float32 [4, 512], replicated, may hold values from -3 to 3
- edge_bias: float32 [512], replicated, may hold values from -3 to 3
- w_message: bfloat16 [512, 512], replicated, may hold values from -0.25 to 0.25
- w_node: bfloat16 [1024, 512], replicated, may hold values from -0.1875 to 0.1875
- w_output: bfloat16 [512, 512], replicated, may hold values from -0.25 to 0.25
- norm_gain: float32 [512], replicated, may hold values from 0.1 to 1.9
- norm_bias: float32 [512], replicated, may hold values from -3 to 3
Outputs:
- mesh_out: bfloat16 [4, 8, 160, 512], P('lat', 'lon')
The draws below stay inside these ranges and needn't reach their ends.
Inputs may be any that keep to these rules, and one draw needn't show every extreme that they name: `receivers`: r // 160 is a neighbour slot s from 0 to 8 (latitude offset s // 3 - 1, longitude offset s % 3 - 1); edges of the first band never name latitude offset -1, those of the last band never +1. For s other than 4, with k = s for s < 4 and k = s - 1 otherwise, the row r % 160 lies in k * 16 to k * 16 + 15 for s = 1, 3, 5, 7 and in k * 16 to k * 16 + 3 for s = 0, 2, 6, 8.
All inputs are finite; a program needn't handle non-finite values.
Results may differ from the reference program's by a relative error of at most 0.0095.
Values may be sent and summed in bfloat16 or wider, within the bound.
No kernel may reach another device: no remote copies, remote signals or barrier semaphores. Data moves between devices by JAX's collectives and lax.ppermute only.
A program may use at most 64 MiB of HBM per device.

```python
import jax
import jax.numpy as jnp
from jax import lax

D = 512
M_DEV = 160
B_SIDE = 16
B_CORNER = 4
G_DEV = 1024
E_DEV = 2048
N_LON = 8
N_LAT = 4


def draw_receivers(key, part):
    base = jax.random.fold_in(key, 11)
    key_slot, key_side, key_corner, key_own = jax.random.split(base, 4)
    array_shape = (N_LAT, N_LON, E_DEV)
    raw_slot = jax.random.randint(key_slot, array_shape, 0, 40)
    neighbour = raw_slot - 32
    neighbour = neighbour + (neighbour >= 4).astype(jnp.int32)
    slot_number = jnp.where(raw_slot < 32, 4, neighbour)
    band_index = jnp.arange(N_LAT, dtype=jnp.int32)[:, None, None]
    lat_offset = slot_number // 3
    outside = (band_index == 0) & (lat_offset == 0) | (band_index == N_LAT - 1) & (lat_offset == 2)
    slot_number = jnp.where(outside, 3 + slot_number % 3, slot_number)
    side_row = jax.random.randint(key_side, array_shape, 0, B_SIDE)
    corner_row = jax.random.randint(key_corner, array_shape, 0, B_CORNER)
    own_row = jax.random.randint(key_own, array_shape, 0, M_DEV)
    strip_number = jnp.where(slot_number < 4, slot_number, slot_number - 1)
    is_corner = (slot_number % 2 == 0) & (slot_number != 4)
    border_row = strip_number * B_SIDE + jnp.where(is_corner, corner_row, side_row)
    row_number = jnp.where(slot_number == 4, own_row, border_row)
    return (slot_number * M_DEV + row_number).astype(jnp.int32)


def plant(drawn, own_key, least, high):
    place = [jax.random.randint(jax.random.fold_in(own_key, axis), (), 0, length) for axis, length in enumerate(drawn.shape)]
    main_axis = drawn.shape.index(max(drawn.shape))
    beside = place[:main_axis] + [(place[main_axis] + 1) % drawn.shape[main_axis]] + place[main_axis + 1:]
    return drawn.at[tuple(place)].set(least).at[tuple(beside)].set(high)


def levels(own_key, dims, cuts, least, top_value):
    level = 1.0
    for position, parts in cuts:
        draws = jax.random.uniform(jax.random.fold_in(jax.random.fold_in(own_key, 6), position), (parts,), jnp.float32, least / len(cuts), top_value / len(cuts))
        level = level * jnp.repeat(jnp.exp(draws), dims[position] // parts).reshape((-1,) + (1,) * (len(dims) - 1 - position))
    return level


def scatter_about(rng, extent, spread, bound, cuts=(), kind=jnp.bfloat16):
    level = levels(rng, extent, cuts, -0.22, 0.18) if cuts else 1.0
    result = jax.random.normal(rng, extent, jnp.float32) * spread * level
    return jnp.minimum(jnp.maximum(result, -bound), bound).astype(kind)


def setup_inputs(seed: int = 0) -> dict:
    seeds = jax.random.split(jax.random.key(seed), 15)
    return {
        "grid_latent": scatter_about(seeds[0], (N_LAT, N_LON, G_DEV, D), 1.0, 6.0, ((0, 4), (1, 8))),
        "mesh_latent": scatter_about(seeds[1], (N_LAT, N_LON, M_DEV, D), 1.0, 6.0, ((0, 4), (1, 8))),
        "edge_geometry": scatter_about(seeds[2], (N_LAT, N_LON, 4, E_DEV), 1.0, 6.0, ((0, 4), (1, 8)), jnp.float32),
        "senders": plant(jax.random.randint(seeds[3], (N_LAT, N_LON, E_DEV), 0, G_DEV), jax.random.fold_in(seeds[3], 1), 0, G_DEV - 1).astype(jnp.int32),
        "receivers": draw_receivers(jax.random.fold_in(seeds[14], 71), 0),
        "w_grid": scatter_about(seeds[5], (D, D), D ** -0.5, 0.25),
        "w_mesh": scatter_about(seeds[6], (D, D), D ** -0.5, 0.25),
        "w_edge": scatter_about(seeds[7], (4, D), 4 ** -0.5, 3.0, (), jnp.float32),
        "edge_bias": scatter_about(seeds[8], (D,), 0.5, 3.0, (), jnp.float32),
        "w_message": scatter_about(seeds[9], (D, D), D ** -0.5, 0.25),
        "w_node": scatter_about(seeds[10], (2 * D, D), (2 * D) ** -0.5, 0.1875),
        "w_output": scatter_about(seeds[11], (D, D), D ** -0.5, 0.25),
        "norm_gain": jnp.clip(1.0 + 0.18 * jax.random.normal(seeds[12], (D,), jnp.float32), 0.1, 1.9),
        "norm_bias": scatter_about(seeds[13], (D,), 0.5, 3.0, (), jnp.float32),
    }


def reference(grid_latent, mesh_latent, edge_geometry, senders, receivers, w_grid, w_mesh, w_edge, edge_bias, w_message, w_node, w_output, norm_gain, norm_bias):
    features = mesh_latent.shape[-1]
    mesh_flat = mesh_latent.reshape(-1, features)
    mesh_proj = jnp.dot(mesh_flat, w_mesh, preferred_element_type=jnp.float32)
    lon_index = jnp.arange(N_LON, dtype=jnp.int32)[:, None]

    def one_band(summed, items):
        band_grid, band_senders, band_receivers, band_geometry, band_index = items
        grid_proj = jnp.dot(band_grid.reshape(-1, features), w_grid, preferred_element_type=jnp.float32)
        grid_proj = grid_proj.reshape(N_LON, G_DEV, features)
        gathered = jax.vmap(lambda table, picks: jnp.take(table, picks, axis=0))(grid_proj, band_senders)
        slot_number = band_receivers // M_DEV
        row_number = band_receivers % M_DEV
        target_lat = band_index + slot_number // 3 - 1
        target_lon = (lon_index + slot_number % 3 - 1) % N_LON
        node_ids = ((target_lat * N_LON + target_lon) * M_DEV + row_number).astype(jnp.int32)
        geometry = jnp.einsum('lce,cd->led', band_geometry, w_edge, precision=lax.Precision.HIGHEST)
        preact = gathered + jnp.take(mesh_proj, node_ids, axis=0) + geometry + edge_bias
        hidden = jax.nn.silu(preact).astype(jnp.bfloat16)
        message = jnp.dot(hidden.reshape(-1, features), w_message, preferred_element_type=jnp.float32).astype(jnp.bfloat16)
        summed = summed + jax.ops.segment_sum(message.astype(jnp.float32), node_ids.reshape(-1), num_segments=mesh_flat.shape[0])
        return (summed, None)
    bands = jnp.arange(N_LAT, dtype=jnp.int32)
    start = jnp.zeros(mesh_flat.shape, jnp.float32)
    aggregated, _ = lax.scan(one_band, start, (grid_latent, senders, receivers, edge_geometry, bands))
    node_in = jnp.concatenate([mesh_flat, aggregated.astype(jnp.bfloat16)], axis=1)
    node_hidden = jax.nn.silu(jnp.dot(node_in, w_node, preferred_element_type=jnp.float32)).astype(jnp.bfloat16)
    update = jnp.dot(node_hidden, w_output, preferred_element_type=jnp.float32)
    row_mean = lax.optimization_barrier(jnp.mean(update, axis=-1, keepdims=True))
    centered = update - row_mean
    row_var = lax.optimization_barrier(jnp.mean(centered * centered, axis=-1, keepdims=True))
    normed = centered * lax.rsqrt(row_var + 1e-05) * norm_gain + norm_bias
    mesh_out = (mesh_flat.astype(jnp.float32) + normed).astype(jnp.bfloat16)
    return mesh_out.reshape(mesh_latent.shape)
```

```python
import functools

import jax
import jax.numpy as jnp
from jax import lax
from jax.experimental import pallas as pl
from jax.experimental.pallas import tpu as pltpu
from jax.sharding import PartitionSpec as P

B_SIDE = 16
B_CORNER = 4
CORNER_ROWS = 8
SEND_ROWS = B_SIDE + 2 * CORNER_ROWS
GEOMETRY_ROWS = 16
side_slots = (5, 3, 1, 7)
corner_slots = (2, 0, 8, 6)
BORDER = len(side_slots) * B_SIDE + len(corner_slots) * B_CORNER

bf16 = jnp.bfloat16
f32 = jnp.float32


def strip_row(slot):
    return (slot if slot < 4 else slot - 1) * B_SIDE


def silu(x):
    half = 0.5 * x
    return half + half * jnp.tanh(half)


def dot(a, b, dims=(((1,), (0,)), ((), ()))):
    return lax.dot_general(a, b, dims, preferred_element_type=f32)


def grid_kernel(senders, grid_rows, w_grid, out, proj, *, block):
    nodes = grid_rows.shape[0]
    proj[...] = dot(grid_rows[...], w_grid[...]).astype(bf16)
    for start in range(0, out.shape[0], block):
        picks = jnp.broadcast_to(senders[:, start : start + block], (128, block)).T
        lane = lax.broadcasted_iota(jnp.int32, (block, 128), 1)
        onehot = jnp.concatenate(
            [(picks - base == lane).astype(f32).astype(bf16) for base in range(0, nodes, 128)],
            axis=1,
        )
        out[start : start + block] = dot(onehot, proj[...])


def edge_kernel(
    grid_term,
    own_mesh,
    from_right,
    from_left,
    from_below,
    from_above,
    targets,
    geometry,
    w_mesh,
    w_edge,
    edge_bias,
    w_message,
    own_sum,
    to_right,
    to_left,
    to_above,
    to_below,
    table,
    factors,
    summed,
    *,
    block,
):
    mesh_rows = own_mesh.shape[0]
    border_end = mesh_rows + BORDER
    received = (from_right, from_left, from_below, from_above)
    table[:mesh_rows] = dot(own_mesh[...], w_mesh[...])
    arrived = dot(jnp.concatenate([ref[...] for ref in received], axis=0), w_mesh[...])
    row = mesh_rows
    for i in range(4):
        table[row : row + B_SIDE] = arrived[i * SEND_ROWS : i * SEND_ROWS + B_SIDE]
        row += B_SIDE
    for i in (2, 3):
        for j in range(2):
            first = i * SEND_ROWS + B_SIDE + j * CORNER_ROWS
            table[row : row + B_CORNER] = arrived[first : first + B_CORNER]
            row += B_CORNER
    w_high = w_edge[...].astype(bf16).astype(f32)
    bias = edge_bias[...]
    bias_high = bias.astype(bf16).astype(f32)
    table[row : row + 4] = w_high
    table[row + 4 : row + 8] = w_edge[...] - w_high
    table[row + 8 : row + 12] = w_high
    table[row + 12 : row + 13] = bias_high
    table[row + 13 : row + 14] = bias - bias_high
    table[row + 14 : row + 16] = jnp.zeros((2, table.shape[1]), f32)
    table_bf16 = table[...].astype(bf16)

    high = geometry[...].astype(bf16).astype(f32)
    factors[0:4] = high
    factors[4:8] = high
    factors[8:12] = geometry[...] - high
    factors[12:14] = jnp.ones((2, factors.shape[1]), f32)
    factors[14:16] = jnp.zeros((2, factors.shape[1]), f32)

    places = {}
    for i, slot in enumerate(side_slots):
        places[slot] = mesh_rows + i * B_SIDE
    for i, slot in enumerate(corner_slots):
        places[slot] = mesh_rows + len(side_slots) * B_SIDE + i * B_CORNER
    named = targets[...]
    shift = jnp.zeros_like(named)
    for slot in range(9):
        base = slot * mesh_rows
        if slot != 4:
            base += strip_row(slot) - places[slot]
        shift = jnp.where(named >= slot * mesh_rows, base, shift)
    index = named - shift

    total = None
    for start in range(0, grid_term.shape[0], block):
        ids = lax.broadcasted_iota(jnp.int32, (border_end, block), 0)
        onehot = (ids == index[:, start : start + block]).astype(f32).astype(bf16)
        picks = jnp.concatenate(
            [onehot, factors[:, start : start + block].astype(bf16)], axis=0
        )
        preact = grid_term[start : start + block] + dot(
            picks, table_bf16, (((0,), (0,)), ((), ()))
        )
        hidden = silu(preact).astype(bf16)
        message = dot(hidden, w_message[...]).astype(bf16)
        added = dot(onehot, message)
        total = added if total is None else total + added
    summed[...] = total
    own_sum[...] = summed[:mesh_rows]
    sent = {}
    for slot in side_slots:
        sent[slot] = summed[places[slot] : places[slot] + B_SIDE]
    pad = jnp.zeros((CORNER_ROWS - B_CORNER, table.shape[1]), f32)
    for slot in corner_slots:
        rows = summed[places[slot] : places[slot] + B_CORNER]
        sent[slot] = jnp.concatenate([rows, pad], axis=0)
    to_right[...] = jnp.concatenate([sent[5], sent[2], sent[8]], axis=0).astype(bf16)
    to_left[...] = jnp.concatenate([sent[3], sent[0], sent[6]], axis=0).astype(bf16)
    to_above[...] = sent[7].astype(bf16)
    to_below[...] = sent[1].astype(bf16)


def node_kernel(
    own_mesh,
    own_sum,
    from_left,
    from_right,
    from_below,
    from_above,
    w_node,
    w_output,
    norm_gain,
    norm_bias,
    out,
    agg,
):
    features = own_mesh.shape[1]
    agg[...] = own_sum[...]
    for ref, slots in ((from_left, (5,)), (from_right, (3,)), (from_below, (7, 8, 6)), (from_above, (1, 2, 0))):
        first = 0
        for slot in slots:
            rows = B_SIDE if slot % 2 else CORNER_ROWS
            place = strip_row(slot)
            agg[place : place + rows] += ref[...].astype(f32)[first : first + rows]
            first += rows
    hidden = dot(own_mesh[...], w_node[:features]) + dot(agg[...].astype(bf16), w_node[features:])
    hidden = silu(hidden).astype(bf16)
    update = dot(hidden, w_output[...])
    mean = jnp.mean(update, axis=-1, keepdims=True)
    centered = update - mean
    var = jnp.mean(centered * centered, axis=-1, keepdims=True)
    normed = centered * lax.rsqrt(var + 1e-05) * norm_gain[...] + norm_bias[...]
    out[...] = (own_mesh[...].astype(f32) + normed).astype(bf16)


def shift_by(block, axis, step, wrap):
    count = lax.axis_size(axis)
    pairs = [(i, (i + step) % count) for i in range(count) if wrap or 0 <= i + step < count]
    return lax.ppermute(block, axis, pairs)


def local(
    grid_latent,
    mesh_latent,
    edge_geometry,
    senders,
    receivers,
    w_grid,
    w_mesh,
    w_edge,
    edge_bias,
    w_message,
    w_node,
    w_output,
    norm_gain,
    norm_bias,
):
    grid_rows = grid_latent[0, 0]
    own_mesh = mesh_latent[0, 0]
    mesh_rows, features = own_mesh.shape
    edges = senders.shape[2]
    block = min(512, edges)
    table_rows = mesh_rows + BORDER + GEOMETRY_ROWS

    def piece(slot, rows):
        return lax.slice_in_dim(own_mesh, strip_row(slot), strip_row(slot) + rows)

    def side(slot):
        return piece(slot, B_SIDE)

    def corner(slot):
        return piece(slot, CORNER_ROWS)

    cat = functools.partial(jnp.concatenate, axis=0)
    from_right = shift_by(cat([side(5), corner(2), corner(8)]), "lon", -1, True)
    from_left = shift_by(cat([side(3), corner(0), corner(6)]), "lon", 1, True)
    mid, end = B_SIDE + CORNER_ROWS, SEND_ROWS
    from_below = shift_by(
        cat([side(1), from_right[B_SIDE:mid], from_left[B_SIDE:mid]]), "lat", 1, False
    )
    from_above = shift_by(
        cat([side(7), from_right[mid:end], from_left[mid:end]]), "lat", -1, False
    )

    grid_term = pl.pallas_call(
        functools.partial(grid_kernel, block=block),
        out_shape=jax.ShapeDtypeStruct((edges, features), f32),
        scratch_shapes=[pltpu.VMEM(grid_rows.shape, bf16)],
        cost_estimate=pl.CostEstimate(flops=6_000_000_000, transcendentals=0, bytes_accessed=6_000_000),
        name="grid_term",
    )(senders[0], grid_rows, w_grid)

    packed = jax.ShapeDtypeStruct((SEND_ROWS, features), bf16)
    strip = jax.ShapeDtypeStruct((B_SIDE, features), bf16)
    own_sum, to_right, to_left, to_above, to_below = pl.pallas_call(
        functools.partial(edge_kernel, block=block),
        out_shape=(jax.ShapeDtypeStruct((mesh_rows, features), f32), packed, packed, strip, strip),
        scratch_shapes=[
            pltpu.VMEM((table_rows, features), f32),
            pltpu.VMEM((GEOMETRY_ROWS, edges), f32),
            pltpu.VMEM((mesh_rows + BORDER, features), f32),
        ],
        name="edge_sums",
    )(
        grid_term,
        own_mesh,
        from_right,
        from_left,
        from_below,
        from_above,
        receivers[0],
        edge_geometry[0, 0],
        w_mesh,
        w_edge,
        edge_bias[None],
        w_message,
    )

    got_left = shift_by(to_right, "lon", 1, True)
    got_right = shift_by(to_left, "lon", -1, True)
    got_below = shift_by(cat([to_above, got_left[mid:end], got_right[mid:end]]), "lat", 1, False)
    got_above = shift_by(
        cat([to_below, got_left[B_SIDE:mid], got_right[B_SIDE:mid]]), "lat", -1, False
    )
    mesh_out = pl.pallas_call(
        node_kernel,
        out_shape=jax.ShapeDtypeStruct(own_mesh.shape, bf16),
        scratch_shapes=[pltpu.VMEM((mesh_rows, features), f32)],
        name="node_update",
    )(
        own_mesh,
        own_sum,
        got_left,
        got_right,
        got_below,
        got_above,
        w_node,
        w_output,
        norm_gain[None],
        norm_bias[None],
    )
    return mesh_out[None, None]


def solution(mesh):
    return jax.shard_map(
        local,
        mesh=mesh,
        in_specs=(
            P("lat", "lon", None, None),
            P("lat", "lon", None, None),
            P("lat", "lon", None, None),
            P("lat", "lon", None),
            P("lat", "lon", None),
            P(),
            P(),
            P(),
            P(),
            P(),
            P(),
            P(),
            P(),
            P(),
        ),
        out_specs=P("lat", "lon", None, None),
        check_vma=False,
    )
```

```python
import functools

import jax
import jax.numpy as jnp
from jax import lax
from jax.experimental import pallas as pl
from jax.experimental.pallas import tpu as pltpu
from jax.sharding import PartitionSpec as P

B_SIDE = 16
B_CORNER = 4
CORNER_ROWS = 8
SEND_ROWS = B_SIDE + 2 * CORNER_ROWS
GEOMETRY_ROWS = 16
side_slots = (5, 3, 1, 7)
corner_slots = (2, 0, 8, 6)
BORDER = len(side_slots) * B_SIDE + len(corner_slots) * B_CORNER

bf16 = jnp.bfloat16
f32 = jnp.float32


def strip_row(slot):
    return (slot if slot < 4 else slot - 1) * B_SIDE


def silu(x):
    half = 0.5 * x
    return half + half * jnp.tanh(half)


def dot(a, b, dims=(((1,), (0,)), ((), ()))):
    return lax.dot_general(a, b, dims, preferred_element_type=f32)


def grid_kernel(senders, grid_rows, w_grid, out, proj, *, block):
    nodes = grid_rows.shape[0]
    proj[...] = dot(grid_rows[...], w_grid[...]).astype(bf16)
    for start in range(0, out.shape[0], block):
        picks = jnp.broadcast_to(senders[:, start : start + block], (128, block)).T
        lane = lax.broadcasted_iota(jnp.int32, (block, 128), 1)
        onehot = jnp.concatenate(
            [(picks - base == lane).astype(f32).astype(bf16) for base in range(0, nodes, 128)],
            axis=1,
        )
        out[start : start + block] = dot(onehot, proj[...])


def edge_kernel(
    grid_term,
    own_mesh,
    from_right,
    from_left,
    from_below,
    from_above,
    targets,
    geometry,
    w_mesh,
    w_edge,
    edge_bias,
    w_message,
    own_sum,
    to_right,
    to_left,
    to_above,
    to_below,
    table,
    factors,
    summed,
    *,
    block,
):
    mesh_rows = own_mesh.shape[0]
    border_end = mesh_rows + BORDER
    received = (from_right, from_left, from_below, from_above)
    table[:mesh_rows] = dot(own_mesh[...], w_mesh[...])
    arrived = dot(jnp.concatenate([ref[...] for ref in received], axis=0), w_mesh[...])
    row = mesh_rows
    for i in range(4):
        table[row : row + B_SIDE] = arrived[i * SEND_ROWS : i * SEND_ROWS + B_SIDE]
        row += B_SIDE
    for i in (2, 3):
        for j in range(2):
            first = i * SEND_ROWS + B_SIDE + j * CORNER_ROWS
            table[row : row + B_CORNER] = arrived[first : first + B_CORNER]
            row += B_CORNER
    w_high = w_edge[...].astype(bf16).astype(f32)
    bias = edge_bias[...]
    bias_high = bias.astype(bf16).astype(f32)
    table[row : row + 4] = w_high
    table[row + 4 : row + 8] = w_edge[...] - w_high
    table[row + 8 : row + 12] = w_high
    table[row + 12 : row + 13] = bias_high
    table[row + 13 : row + 14] = bias - bias_high
    table[row + 14 : row + 16] = jnp.zeros((2, table.shape[1]), f32)
    table_bf16 = table[...].astype(bf16)

    high = geometry[...].astype(bf16).astype(f32)
    factors[0:4] = high
    factors[4:8] = high
    factors[8:12] = geometry[...] - high
    factors[12:14] = jnp.ones((2, factors.shape[1]), f32)
    factors[14:16] = jnp.zeros((2, factors.shape[1]), f32)

    places = {}
    for i, slot in enumerate(side_slots):
        places[slot] = mesh_rows + i * B_SIDE
    for i, slot in enumerate(corner_slots):
        places[slot] = mesh_rows + len(side_slots) * B_SIDE + i * B_CORNER
    named = targets[...]
    shift = jnp.zeros_like(named)
    for slot in range(9):
        base = slot * mesh_rows
        if slot != 4:
            base += strip_row(slot) - places[slot]
        shift = jnp.where(named >= slot * mesh_rows, base, shift)
    index = named - shift

    total = None
    for start in range(0, grid_term.shape[0], block):
        ids = lax.broadcasted_iota(jnp.int32, (border_end, block), 0)
        onehot = (ids == index[:, start : start + block]).astype(f32).astype(bf16)
        picks = jnp.concatenate(
            [onehot, factors[:, start : start + block].astype(bf16)], axis=0
        )
        preact = grid_term[start : start + block] + dot(
            picks, table_bf16, (((0,), (0,)), ((), ()))
        )
        hidden = silu(preact).astype(bf16)
        message = dot(hidden, w_message[...]).astype(bf16)
        added = dot(onehot, message)
        total = added if total is None else total + added
    summed[...] = total
    own_sum[...] = summed[:mesh_rows]
    sent = {}
    for slot in side_slots:
        sent[slot] = summed[places[slot] : places[slot] + B_SIDE]
    pad = jnp.zeros((CORNER_ROWS - B_CORNER, table.shape[1]), f32)
    for slot in corner_slots:
        rows = summed[places[slot] : places[slot] + B_CORNER]
        sent[slot] = jnp.concatenate([rows, pad], axis=0)
    to_right[...] = jnp.concatenate([sent[5], sent[2], sent[8]], axis=0).astype(bf16)
    to_left[...] = jnp.concatenate([sent[3], sent[0], sent[6]], axis=0).astype(bf16)
    to_above[...] = sent[7].astype(bf16)
    to_below[...] = sent[1].astype(bf16)


def node_kernel(
    own_mesh,
    own_sum,
    from_left,
    from_right,
    from_below,
    from_above,
    w_node,
    w_output,
    norm_gain,
    norm_bias,
    out,
    agg,
):
    features = own_mesh.shape[1]
    agg[...] = own_sum[...]
    for ref, slots in ((from_left, (5,)), (from_right, (3,)), (from_below, (7, 8, 6)), (from_above, (1, 2, 0))):
        first = 0
        for slot in slots:
            rows = B_SIDE if slot % 2 else CORNER_ROWS
            place = strip_row(slot)
            agg[place : place + rows] += ref[...].astype(f32)[first : first + rows]
            first += rows
    hidden = dot(own_mesh[...], w_node[:features]) + dot(agg[...].astype(bf16), w_node[features:])
    hidden = silu(hidden).astype(bf16)
    update = dot(hidden, w_output[...])
    mean = jnp.mean(update, axis=-1, keepdims=True)
    centered = update - mean
    var = jnp.mean(centered * centered, axis=-1, keepdims=True)
    normed = centered * lax.rsqrt(var + 1e-05) * norm_gain[...] + norm_bias[...]
    out[...] = (own_mesh[...].astype(f32) + normed).astype(bf16)


def pack_sides_kernel(own_mesh, to_left, to_right):
    for out, slots in ((to_left, (5, 2, 8)), (to_right, (3, 0, 6))):
        pieces = [
            own_mesh[strip_row(slot) : strip_row(slot) + (B_SIDE if slot % 2 else CORNER_ROWS)]
            for slot in slots
        ]
        out[...] = jnp.concatenate(pieces, axis=0)


def pack_bands_kernel(
    up_side, down_side, from_right, from_left, to_above, to_below, *, up_row, down_row, up_first
):
    first, second = B_SIDE, B_SIDE + CORNER_ROWS
    up, down = (first, second) if up_first else (second, first)
    for out, side, row, corner in (
        (to_above, up_side, up_row, up),
        (to_below, down_side, down_row, down),
    ):
        out[:B_SIDE] = side[row : row + B_SIDE]
        for i, ref in enumerate((from_right, from_left)):
            place = B_SIDE + i * CORNER_ROWS
            out[place : place + CORNER_ROWS] = ref[corner : corner + CORNER_ROWS]


def on_chip(x):
    return pltpu.with_memory_space_constraint(x, pltpu.VMEM)


def call(kernel, name, outs, args, scratch=(), flops=0):
    cost = pl.CostEstimate(flops=flops, transcendentals=0, bytes_accessed=0) if flops else None
    return pl.pallas_call(
        kernel,
        out_shape=tuple(pltpu.VMEM(shape, dtype) for shape, dtype in outs),
        scratch_shapes=list(scratch),
        cost_estimate=cost,
        compiler_params=pltpu.CompilerParams(vmem_limit_bytes=24 * 2**20),
        name=name,
    )(*(on_chip(x) for x in args))


def shift_by(block, axis, step):
    count = lax.axis_size(axis)
    return lax.ppermute(block, axis, [(i, (i + step) % count) for i in range(count)])


def local(
    grid_latent,
    mesh_latent,
    edge_geometry,
    senders,
    receivers,
    w_grid,
    w_mesh,
    w_edge,
    edge_bias,
    w_message,
    w_node,
    w_output,
    norm_gain,
    norm_bias,
):
    grid_rows = grid_latent[0, 0]
    own_mesh = mesh_latent[0, 0]
    mesh_rows, features = own_mesh.shape
    edges = senders.shape[2]
    block = min(512, edges)
    table_rows = mesh_rows + BORDER + GEOMETRY_ROWS

    packed = ((SEND_ROWS, features), bf16)
    strip = ((B_SIDE, features), bf16)

    to_left, to_right = call(pack_sides_kernel, "pack_sides", (packed, packed), (own_mesh,))
    from_right = shift_by(to_left, "lon", -1)
    from_left = shift_by(to_right, "lon", 1)
    to_above, to_below = call(
        functools.partial(
            pack_bands_kernel, up_row=strip_row(1), down_row=strip_row(7), up_first=True
        ),
        "pack_bands",
        (packed, packed),
        (own_mesh, own_mesh, from_right, from_left),
    )
    from_below = shift_by(to_above, "lat", 1)
    from_above = shift_by(to_below, "lat", -1)

    (grid_term,) = call(
        functools.partial(grid_kernel, block=block),
        "grid_term",
        (((edges, features), f32),),
        (senders[0], grid_rows, w_grid),
        [pltpu.VMEM(grid_rows.shape, bf16)],
        flops=6_000_000_000,
    )
    own_sum, to_right, to_left, to_above, to_below = call(
        functools.partial(edge_kernel, block=block),
        "edge_sums",
        ((own_mesh.shape, f32), packed, packed, strip, strip),
        (
            grid_term,
            own_mesh,
            from_right,
            from_left,
            from_below,
            from_above,
            receivers[0],
            edge_geometry[0, 0],
            w_mesh,
            w_edge,
            edge_bias[None],
            w_message,
        ),
        [
            pltpu.VMEM((table_rows, features), f32),
            pltpu.VMEM((GEOMETRY_ROWS, edges), f32),
            pltpu.VMEM((mesh_rows + BORDER, features), f32),
        ],
    )

    got_left = shift_by(to_right, "lon", 1)
    got_right = shift_by(to_left, "lon", -1)
    to_above, to_below = call(
        functools.partial(pack_bands_kernel, up_row=0, down_row=0, up_first=False),
        "pack_sums",
        (packed, packed),
        (to_above, to_below, got_left, got_right),
    )
    got_below = shift_by(to_above, "lat", 1)
    got_above = shift_by(to_below, "lat", -1)
    (mesh_out,) = call(
        node_kernel,
        "node_update",
        ((own_mesh.shape, bf16),),
        (
            own_mesh,
            own_sum,
            got_left,
            got_right,
            got_below,
            got_above,
            w_node,
            w_output,
            norm_gain[None],
            norm_bias[None],
        ),
        [pltpu.VMEM((mesh_rows, features), f32)],
    )
    return mesh_out[None, None]


def solution(mesh):
    return jax.shard_map(
        local,
        mesh=mesh,
        in_specs=(
            P("lat", "lon", None, None),
            P("lat", "lon", None, None),
            P("lat", "lon", None, None),
            P("lat", "lon", None),
            P("lat", "lon", None),
            P(),
            P(),
            P(),
            P(),
            P(),
            P(),
            P(),
            P(),
            P(),
        ),
        out_specs=P("lat", "lon", None, None),
        check_vma=False,
    )
```

```python
import functools

import jax
import jax.numpy as jnp
from jax import lax
from jax.experimental import pallas as pl
from jax.experimental.pallas import tpu as pltpu
from jax.sharding import PartitionSpec as P

B_SIDE = 16
B_CORNER = 4
CORNER_ROWS = 8
SEND_ROWS = B_SIDE + 2 * CORNER_ROWS
GEOMETRY_ROWS = 16
side_slots = (5, 3, 1, 7)
corner_slots = (2, 0, 8, 6)
BORDER = len(side_slots) * B_SIDE + len(corner_slots) * B_CORNER

bf16 = jnp.bfloat16
f32 = jnp.float32


def strip_row(slot):
    return (slot if slot < 4 else slot - 1) * B_SIDE


def silu(x):
    half = 0.5 * x
    return half + half * jnp.tanh(half)


def dot(a, b, dims=(((1,), (0,)), ((), ()))):
    return lax.dot_general(a, b, dims, preferred_element_type=f32)


def first_grid_kernel(senders, grid_rows, w_grid, packed, out, proj, *, block):
    del packed
    proj[...] = dot(grid_rows[...], w_grid[...]).astype(bf16)
    grid_kernel(senders, proj, out, block=block, offset=0)


def grid_kernel(senders, proj, out, *, block, offset):
    nodes = proj.shape[0]
    for start in range(0, out.shape[0], block):
        picks = jnp.broadcast_to(senders[:, offset + start : offset + start + block], (128, block)).T
        lane = lax.broadcasted_iota(jnp.int32, (block, 128), 1)
        onehot = jnp.concatenate(
            [(picks - base == lane).astype(f32).astype(bf16) for base in range(0, nodes, 128)],
            axis=1,
        )
        out[start : start + block] = dot(onehot, proj[...])


def edge_kernel(
    grid_first,
    grid_second,
    own_mesh,
    from_right,
    from_left,
    from_below,
    from_above,
    targets,
    geometry,
    w_mesh,
    w_edge,
    edge_bias,
    w_message,
    own_sum,
    to_right,
    to_left,
    to_above,
    to_below,
    table,
    factors,
    summed,
    *,
    block,
):
    mesh_rows = own_mesh.shape[0]
    border_end = mesh_rows + BORDER
    received = (from_right, from_left, from_below, from_above)
    table[:mesh_rows] = dot(own_mesh[...], w_mesh[...])
    arrived = dot(jnp.concatenate([ref[...] for ref in received], axis=0), w_mesh[...])
    row = mesh_rows
    for i in range(4):
        table[row : row + B_SIDE] = arrived[i * SEND_ROWS : i * SEND_ROWS + B_SIDE]
        row += B_SIDE
    for i in (2, 3):
        for j in range(2):
            first = i * SEND_ROWS + B_SIDE + j * CORNER_ROWS
            table[row : row + B_CORNER] = arrived[first : first + B_CORNER]
            row += B_CORNER
    w_high = w_edge[...].astype(bf16).astype(f32)
    bias = edge_bias[...]
    bias_high = bias.astype(bf16).astype(f32)
    table[row : row + 4] = w_high
    table[row + 4 : row + 8] = w_edge[...] - w_high
    table[row + 8 : row + 12] = w_high
    table[row + 12 : row + 13] = bias_high
    table[row + 13 : row + 14] = bias - bias_high
    table[row + 14 : row + 16] = jnp.zeros((2, table.shape[1]), f32)
    table_bf16 = table[...].astype(bf16)

    high = geometry[...].astype(bf16).astype(f32)
    factors[0:4] = high
    factors[4:8] = high
    factors[8:12] = geometry[...] - high
    factors[12:14] = jnp.ones((2, factors.shape[1]), f32)
    factors[14:16] = jnp.zeros((2, factors.shape[1]), f32)

    places = {}
    for i, slot in enumerate(side_slots):
        places[slot] = mesh_rows + i * B_SIDE
    for i, slot in enumerate(corner_slots):
        places[slot] = mesh_rows + len(side_slots) * B_SIDE + i * B_CORNER
    named = targets[...]
    shift = jnp.zeros_like(named)
    for slot in range(9):
        base = slot * mesh_rows
        if slot != 4:
            base += strip_row(slot) - places[slot]
        shift = jnp.where(named >= slot * mesh_rows, base, shift)
    index = named - shift

    total = None
    split = grid_first.shape[0]
    for start in range(0, targets.shape[1], block):
        grid_term = grid_first if start < split else grid_second
        row = start if start < split else start - split
        ids = lax.broadcasted_iota(jnp.int32, (border_end, block), 0)
        onehot = (ids == index[:, start : start + block]).astype(f32).astype(bf16)
        picks = jnp.concatenate(
            [onehot, factors[:, start : start + block].astype(bf16)], axis=0
        )
        preact = grid_term[row : row + block] + dot(
            picks, table_bf16, (((0,), (0,)), ((), ()))
        )
        hidden = silu(preact).astype(bf16)
        message = dot(hidden, w_message[...]).astype(bf16)
        added = dot(onehot, message)
        total = added if total is None else total + added
    summed[...] = total
    own_sum[...] = summed[:mesh_rows]
    sent = {}
    for slot in side_slots:
        sent[slot] = summed[places[slot] : places[slot] + B_SIDE]
    pad = jnp.zeros((CORNER_ROWS - B_CORNER, table.shape[1]), f32)
    for slot in corner_slots:
        rows = summed[places[slot] : places[slot] + B_CORNER]
        sent[slot] = jnp.concatenate([rows, pad], axis=0)
    to_right[...] = jnp.concatenate([sent[5], sent[2], sent[8]], axis=0).astype(bf16)
    to_left[...] = jnp.concatenate([sent[3], sent[0], sent[6]], axis=0).astype(bf16)
    to_above[...] = sent[7].astype(bf16)
    to_below[...] = sent[1].astype(bf16)


def node_kernel(
    own_mesh,
    own_sum,
    from_left,
    from_right,
    from_below,
    from_above,
    w_node,
    w_output,
    norm_gain,
    norm_bias,
    out,
    agg,
):
    features = own_mesh.shape[1]
    agg[...] = own_sum[...]
    for ref, slots in ((from_left, (5,)), (from_right, (3,)), (from_below, (7, 8, 6)), (from_above, (1, 2, 0))):
        first = 0
        for slot in slots:
            rows = B_SIDE if slot % 2 else CORNER_ROWS
            place = strip_row(slot)
            agg[place : place + rows] += ref[...].astype(f32)[first : first + rows]
            first += rows
    hidden = dot(own_mesh[...], w_node[:features]) + dot(agg[...].astype(bf16), w_node[features:])
    hidden = silu(hidden).astype(bf16)
    update = dot(hidden, w_output[...])
    mean = jnp.mean(update, axis=-1, keepdims=True)
    centered = update - mean
    var = jnp.mean(centered * centered, axis=-1, keepdims=True)
    normed = centered * lax.rsqrt(var + 1e-05) * norm_gain[...] + norm_bias[...]
    out[...] = (own_mesh[...].astype(f32) + normed).astype(bf16)


def pack_sides_kernel(own_mesh, to_left, to_right, low_side, high_side, sems):
    copies = []
    for out, slots in (
        (to_left, (5, 2, 8)),
        (to_right, (3, 0, 6)),
        (low_side, (1,)),
        (high_side, (7,)),
    ):
        place = 0
        for slot in slots:
            rows = B_SIDE if slot % 2 else CORNER_ROWS
            copies.append(
                pltpu.make_async_copy(
                    own_mesh.at[pl.ds(strip_row(slot), rows)],
                    out.at[pl.ds(place, rows)],
                    sems.at[len(copies)],
                )
            )
            place += rows
    for copy in copies:
        copy.start()
    for copy in copies:
        copy.wait()


def pack_bands_kernel(
    up_side, down_side, from_right, from_left, *rest, up_first
):
    to_above, to_below = rest[-2:]
    first, second = B_SIDE, B_SIDE + CORNER_ROWS
    up, down = (first, second) if up_first else (second, first)
    for out, side, corner in ((to_above, up_side, up), (to_below, down_side, down)):
        out[:B_SIDE] = side[...]
        for i, ref in enumerate((from_right, from_left)):
            place = B_SIDE + i * CORNER_ROWS
            out[place : place + CORNER_ROWS] = ref[corner : corner + CORNER_ROWS]


def on_chip(x):
    return pltpu.with_memory_space_constraint(x, pltpu.VMEM)


def call(kernel, name, outs, args, scratch=(), flops=0, on_vmem=True):
    cost = pl.CostEstimate(flops=flops, transcendentals=0, bytes_accessed=0) if flops else None
    return pl.pallas_call(
        kernel,
        out_shape=tuple(
            pltpu.VMEM(shape, dtype) if on_vmem else jax.ShapeDtypeStruct(shape, dtype)
            for shape, dtype in outs
        ),
        scratch_shapes=list(scratch),
        cost_estimate=cost,
        compiler_params=pltpu.CompilerParams(vmem_limit_bytes=24 * 2**20),
        name=name,
    )(*(on_chip(x) for x in args))


def shift_by(block, axis, step):
    count = lax.axis_size(axis)
    return lax.ppermute(block, axis, [(i, (i + step) % count) for i in range(count)])


def local(
    grid_latent,
    mesh_latent,
    edge_geometry,
    senders,
    receivers,
    w_grid,
    w_mesh,
    w_edge,
    edge_bias,
    w_message,
    w_node,
    w_output,
    norm_gain,
    norm_bias,
):
    grid_rows = grid_latent[0, 0]
    own_mesh = mesh_latent[0, 0]
    mesh_rows, features = own_mesh.shape
    edges = senders.shape[2]
    block = min(512, edges // 2)
    table_rows = mesh_rows + BORDER + GEOMETRY_ROWS

    packed = ((SEND_ROWS, features), bf16)
    strip = ((B_SIDE, features), bf16)

    to_left, to_right, low_side, high_side = pl.pallas_call(
        pack_sides_kernel,
        in_specs=[pl.BlockSpec(memory_space=pl.ANY)],
        out_shape=tuple(pltpu.VMEM(shape, dtype) for shape, dtype in (packed, packed, strip, strip)),
        scratch_shapes=[pltpu.SemaphoreType.DMA((8,))],
        cost_estimate=pl.CostEstimate(flops=6_000_000_000, transcendentals=0, bytes_accessed=0),
        compiler_params=pltpu.CompilerParams(vmem_limit_bytes=24 * 2**20),
        name="pack_sides",
    )(pltpu.with_memory_space_constraint(own_mesh, pltpu.HBM))
    from_right = shift_by(to_left, "lon", -1)
    from_left = shift_by(to_right, "lon", 1)
    first_edges = max(edges // 2, 1)
    grid_first, proj = call(
        functools.partial(first_grid_kernel, block=min(block, first_edges)),
        "grid_first",
        (((first_edges, features), f32), (grid_rows.shape, bf16)),
        (senders[0], grid_rows, w_grid, to_left),
        flops=3_000_000_000,
    )
    to_above, to_below = call(
        functools.partial(pack_bands_kernel, up_first=True),
        "pack_bands",
        (packed, packed),
        (low_side, high_side, from_right, from_left, grid_first),
    )
    from_below = shift_by(to_above, "lat", 1)
    from_above = shift_by(to_below, "lat", -1)
    (grid_second,) = call(
        functools.partial(grid_kernel, block=block, offset=first_edges),
        "grid_second",
        (((edges - first_edges, features), f32),),
        (senders[0], proj),
        flops=3_000_000_000,
    )
    own_sum, to_right, to_left, to_above, to_below = call(
        functools.partial(edge_kernel, block=block),
        "edge_sums",
        ((own_mesh.shape, f32), packed, packed, strip, strip),
        (
            grid_first,
            grid_second,
            own_mesh,
            from_right,
            from_left,
            from_below,
            from_above,
            receivers[0],
            edge_geometry[0, 0],
            w_mesh,
            w_edge,
            edge_bias[None],
            w_message,
        ),
        [
            pltpu.VMEM((table_rows, features), f32),
            pltpu.VMEM((GEOMETRY_ROWS, edges), f32),
            pltpu.VMEM((mesh_rows + BORDER, features), f32),
        ],
    )

    got_left = shift_by(to_right, "lon", 1)
    got_right = shift_by(to_left, "lon", -1)
    to_above, to_below = call(
        functools.partial(pack_bands_kernel, up_first=False),
        "pack_sums",
        (packed, packed),
        (to_above, to_below, got_left, got_right),
    )
    got_below = shift_by(to_above, "lat", 1)
    got_above = shift_by(to_below, "lat", -1)
    (mesh_out,) = call(
        node_kernel,
        "node_update",
        ((own_mesh.shape, bf16),),
        (
            own_mesh,
            own_sum,
            got_left,
            got_right,
            got_below,
            got_above,
            w_node,
            w_output,
            norm_gain[None],
            norm_bias[None],
        ),
        [pltpu.VMEM((mesh_rows, features), f32)],
        on_vmem=False,
    )
    return mesh_out[None, None]


def solution(mesh):
    return jax.shard_map(
        local,
        mesh=mesh,
        in_specs=(
            P("lat", "lon", None, None),
            P("lat", "lon", None, None),
            P("lat", "lon", None, None),
            P("lat", "lon", None),
            P("lat", "lon", None),
            P(),
            P(),
            P(),
            P(),
            P(),
            P(),
            P(),
            P(),
            P(),
        ),
        out_specs=P("lat", "lon", None, None),
        check_vma=False,
    )
```

```python
import functools

import jax
import jax.numpy as jnp
from jax import lax
from jax.experimental import pallas as pl
from jax.experimental.pallas import tpu as pltpu
from jax.sharding import PartitionSpec as P

B_SIDE = 16
B_CORNER = 4
CORNER_ROWS = 8
SEND_ROWS = B_SIDE + 2 * CORNER_ROWS
GEOMETRY_ROWS = 16
side_slots = (5, 3, 1, 7)
corner_slots = (2, 0, 8, 6)
BORDER = len(side_slots) * B_SIDE + len(corner_slots) * B_CORNER

bf16 = jnp.bfloat16
f32 = jnp.float32


def strip_row(slot):
    return (slot if slot < 4 else slot - 1) * B_SIDE


def partner_row(even_slot, odd_slot):
    odd = lax.axis_index("lon") % 2
    low, high = strip_row(even_slot), strip_row(odd_slot)
    return pl.multiple_of(low + odd * (high - low), CORNER_ROWS)


def silu(x):
    half = 0.5 * x
    return half + half * jnp.tanh(half)


def dot(a, b, dims=(((1,), (0,)), ((), ()))):
    return lax.dot_general(a, b, dims, preferred_element_type=f32)


def first_grid_kernel(senders, grid_rows, w_grid, packed, out, proj, *, block):
    del packed
    proj[...] = dot(grid_rows[...], w_grid[...]).astype(bf16)
    grid_kernel(senders, proj, out, block=block, offset=0)


def grid_kernel(senders, proj, out, *, block, offset):
    nodes = proj.shape[0]
    for start in range(0, out.shape[0], block):
        picks = jnp.broadcast_to(senders[:, offset + start : offset + start + block], (128, block)).T
        lane = lax.broadcasted_iota(jnp.int32, (block, 128), 1)
        onehot = jnp.concatenate(
            [(picks - base == lane).astype(f32).astype(bf16) for base in range(0, nodes, 128)],
            axis=1,
        )
        out[start : start + block] = dot(onehot, proj[...])


def edge_kernel(
    grid_first,
    grid_second,
    own_mesh,
    from_first,
    from_second,
    from_below,
    from_above,
    targets,
    geometry,
    w_mesh,
    w_edge,
    edge_bias,
    w_message,
    own_sum,
    to_right,
    to_left,
    to_above,
    to_below,
    table,
    factors,
    summed,
    *,
    block,
):
    mesh_rows = own_mesh.shape[0]
    border_end = mesh_rows + BORDER
    received = (from_first, from_second, from_below, from_above)
    table[:mesh_rows] = dot(own_mesh[...], w_mesh[...])
    arrived = dot(jnp.concatenate([ref[...] for ref in received], axis=0), w_mesh[...])
    row = mesh_rows
    for i in range(4):
        table[row : row + B_SIDE] = arrived[i * SEND_ROWS : i * SEND_ROWS + B_SIDE]
        row += B_SIDE
    for i in (2, 3):
        for j in range(2):
            first = i * SEND_ROWS + B_SIDE + j * CORNER_ROWS
            table[row : row + B_CORNER] = arrived[first : first + B_CORNER]
            row += B_CORNER
    w_high = w_edge[...].astype(bf16).astype(f32)
    bias = edge_bias[...]
    bias_high = bias.astype(bf16).astype(f32)
    table[row : row + 4] = w_high
    table[row + 4 : row + 8] = w_edge[...] - w_high
    table[row + 8 : row + 12] = w_high
    table[row + 12 : row + 13] = bias_high
    table[row + 13 : row + 14] = bias - bias_high
    table[row + 14 : row + 16] = jnp.zeros((2, table.shape[1]), f32)
    table_bf16 = table[...].astype(bf16)

    high = geometry[...].astype(bf16).astype(f32)
    factors[0:4] = high
    factors[4:8] = high
    factors[8:12] = geometry[...] - high
    factors[12:14] = jnp.ones((2, factors.shape[1]), f32)
    factors[14:16] = jnp.zeros((2, factors.shape[1]), f32)

    places = {}
    for i, slot in enumerate(side_slots):
        places[slot] = mesh_rows + i * B_SIDE
    for i, slot in enumerate(corner_slots):
        places[slot] = mesh_rows + len(side_slots) * B_SIDE + i * B_CORNER
    named = targets[...]
    odd = lax.axis_index("lon") % 2
    shift = jnp.zeros_like(named)
    for slot in range(9):
        base = slot * mesh_rows
        if slot != 4:
            mirrored = slot // 3 * 3 + 2 - slot % 3
            base += strip_row(slot) - places[slot] + odd * (places[slot] - places[mirrored])
        shift = jnp.where(named >= slot * mesh_rows, base, shift)
    index = named - shift

    total = None
    split = grid_first.shape[0]
    for start in range(0, targets.shape[1], block):
        grid_term = grid_first if start < split else grid_second
        row = start if start < split else start - split
        ids = lax.broadcasted_iota(jnp.int32, (border_end, block), 0)
        onehot = (ids == index[:, start : start + block]).astype(f32).astype(bf16)
        picks = jnp.concatenate(
            [onehot, factors[:, start : start + block].astype(bf16)], axis=0
        )
        preact = grid_term[row : row + block] + dot(
            picks, table_bf16, (((0,), (0,)), ((), ()))
        )
        hidden = silu(preact).astype(bf16)
        message = dot(hidden, w_message[...]).astype(bf16)
        added = dot(onehot, message)
        total = added if total is None else total + added
    summed[...] = total
    own_sum[...] = summed[:mesh_rows]
    sent = {}
    for slot in side_slots:
        sent[slot] = summed[places[slot] : places[slot] + B_SIDE]
    pad = jnp.zeros((CORNER_ROWS - B_CORNER, table.shape[1]), f32)
    for slot in corner_slots:
        rows = summed[places[slot] : places[slot] + B_CORNER]
        sent[slot] = jnp.concatenate([rows, pad], axis=0)
    to_right[...] = jnp.concatenate([sent[5], sent[2], sent[8]], axis=0).astype(bf16)
    to_left[...] = jnp.concatenate([sent[3], sent[0], sent[6]], axis=0).astype(bf16)
    to_above[...] = sent[7].astype(bf16)
    to_below[...] = sent[1].astype(bf16)


def node_kernel(
    own_mesh,
    own_sum,
    from_first,
    from_second,
    from_below,
    from_above,
    w_node,
    w_output,
    norm_gain,
    norm_bias,
    out,
    agg,
):
    features = own_mesh.shape[1]
    agg[...] = own_sum[...]
    for ref, places in (
        (from_first, (partner_row(3, 5),)),
        (from_second, (partner_row(5, 3),)),
        (from_below, (strip_row(7), partner_row(6, 8), partner_row(8, 6))),
        (from_above, (strip_row(1), partner_row(0, 2), partner_row(2, 0))),
    ):
        first = 0
        for i, place in enumerate(places):
            rows = CORNER_ROWS if i else B_SIDE
            agg[pl.ds(place, rows)] += ref[...].astype(f32)[first : first + rows]
            first += rows
    hidden = dot(own_mesh[...], w_node[:features]) + dot(agg[...].astype(bf16), w_node[features:])
    hidden = silu(hidden).astype(bf16)
    update = dot(hidden, w_output[...])
    mean = jnp.mean(update, axis=-1, keepdims=True)
    centered = update - mean
    var = jnp.mean(centered * centered, axis=-1, keepdims=True)
    normed = centered * lax.rsqrt(var + 1e-05) * norm_gain[...] + norm_bias[...]
    out[...] = (own_mesh[...].astype(f32) + normed).astype(bf16)


def pack_sides_kernel(own_mesh, to_first, to_second, low_side, high_side, sems):
    rows_of = (
        (to_first, [partner_row(3, 5), partner_row(0, 2), partner_row(6, 8)]),
        (to_second, [partner_row(5, 3), partner_row(2, 0), partner_row(8, 6)]),
        (low_side, [strip_row(1)]),
        (high_side, [strip_row(7)]),
    )
    copies = []
    for out, sources in rows_of:
        place = 0
        for i, source in enumerate(sources):
            rows = CORNER_ROWS if i else B_SIDE
            copies.append(
                pltpu.make_async_copy(
                    own_mesh.at[pl.ds(source, rows)],
                    out.at[pl.ds(place, rows)],
                    sems.at[len(copies)],
                )
            )
            place += rows
    for copy in copies:
        copy.start()
    for copy in copies:
        copy.wait()


def pack_bands_kernel(
    up_side, down_side, from_first, from_second, *rest, up_first
):
    to_above, to_below = rest[-2:]
    first, second = B_SIDE, B_SIDE + CORNER_ROWS
    up, down = (first, second) if up_first else (second, first)
    for out, side, corner in ((to_above, up_side, up), (to_below, down_side, down)):
        out[:B_SIDE] = side[...]
        for i, ref in enumerate((from_first, from_second)):
            place = B_SIDE + i * CORNER_ROWS
            out[place : place + CORNER_ROWS] = ref[corner : corner + CORNER_ROWS]


def on_chip(x):
    return pltpu.with_memory_space_constraint(x, pltpu.VMEM)


def call(kernel, name, outs, args, scratch=(), flops=0, on_vmem=True):
    cost = pl.CostEstimate(flops=flops, transcendentals=0, bytes_accessed=0) if flops else None
    return pl.pallas_call(
        kernel,
        out_shape=tuple(
            pltpu.VMEM(shape, dtype) if on_vmem else jax.ShapeDtypeStruct(shape, dtype)
            for shape, dtype in outs
        ),
        scratch_shapes=list(scratch),
        cost_estimate=cost,
        compiler_params=pltpu.CompilerParams(vmem_limit_bytes=24 * 2**20),
        name=name,
    )(*(on_chip(x) for x in args))


def shift_by(block, axis, step):
    count = lax.axis_size(axis)
    return lax.ppermute(block, axis, [(i, (i + step) % count) for i in range(count)])


def swap(block, axis, start):
    count = lax.axis_size(axis)
    pairs = []
    for i in range(start, count, 2):
        pairs += [(i, (i + 1) % count), ((i + 1) % count, i)]
    return lax.ppermute(block, axis, pairs)


def local(
    grid_latent,
    mesh_latent,
    edge_geometry,
    senders,
    receivers,
    w_grid,
    w_mesh,
    w_edge,
    edge_bias,
    w_message,
    w_node,
    w_output,
    norm_gain,
    norm_bias,
):
    grid_rows = grid_latent[0, 0]
    own_mesh = mesh_latent[0, 0]
    mesh_rows, features = own_mesh.shape
    edges = senders.shape[2]
    block = min(512, edges // 2)
    table_rows = mesh_rows + BORDER + GEOMETRY_ROWS

    packed = ((SEND_ROWS, features), bf16)
    strip = ((B_SIDE, features), bf16)

    to_left, to_right, low_side, high_side = pl.pallas_call(
        pack_sides_kernel,
        in_specs=[pl.BlockSpec(memory_space=pl.ANY)],
        out_shape=tuple(pltpu.VMEM(shape, dtype) for shape, dtype in (packed, packed, strip, strip)),
        scratch_shapes=[pltpu.SemaphoreType.DMA((8,))],
        cost_estimate=pl.CostEstimate(flops=6_000_000_000, transcendentals=0, bytes_accessed=0),
        compiler_params=pltpu.CompilerParams(vmem_limit_bytes=24 * 2**20),
        name="pack_sides",
    )(pltpu.with_memory_space_constraint(own_mesh, pltpu.HBM))
    from_first = swap(to_left, "lon", 0)
    from_second = swap(to_right, "lon", 1)
    first_edges = max(edges // 2, 1)
    grid_first, proj = call(
        functools.partial(first_grid_kernel, block=min(block, first_edges)),
        "grid_first",
        (((first_edges, features), f32), (grid_rows.shape, bf16)),
        (senders[0], grid_rows, w_grid, to_left),
        flops=3_000_000_000,
    )
    to_above, to_below = call(
        functools.partial(pack_bands_kernel, up_first=True),
        "pack_bands",
        (packed, packed),
        (low_side, high_side, from_first, from_second, grid_first),
    )
    from_below = shift_by(to_above, "lat", 1)
    from_above = shift_by(to_below, "lat", -1)
    (grid_second,) = call(
        functools.partial(grid_kernel, block=block, offset=first_edges),
        "grid_second",
        (((edges - first_edges, features), f32),),
        (senders[0], proj),
        flops=3_000_000_000,
    )
    own_sum, to_right, to_left, to_above, to_below = call(
        functools.partial(edge_kernel, block=block),
        "edge_sums",
        ((own_mesh.shape, f32), packed, packed, strip, strip),
        (
            grid_first,
            grid_second,
            own_mesh,
            from_first,
            from_second,
            from_below,
            from_above,
            receivers[0],
            edge_geometry[0, 0],
            w_mesh,
            w_edge,
            edge_bias[None],
            w_message,
        ),
        [
            pltpu.VMEM((table_rows, features), f32),
            pltpu.VMEM((GEOMETRY_ROWS, edges), f32),
            pltpu.VMEM((mesh_rows + BORDER, features), f32),
        ],
    )

    got_first = swap(to_right, "lon", 0)
    got_second = swap(to_left, "lon", 1)
    to_above, to_below = call(
        functools.partial(pack_bands_kernel, up_first=False),
        "pack_sums",
        (packed, packed),
        (to_above, to_below, got_first, got_second),
    )
    got_below = shift_by(to_above, "lat", 1)
    got_above = shift_by(to_below, "lat", -1)
    (mesh_out,) = call(
        node_kernel,
        "node_update",
        ((own_mesh.shape, bf16),),
        (
            own_mesh,
            own_sum,
            got_first,
            got_second,
            got_below,
            got_above,
            w_node,
            w_output,
            norm_gain[None],
            norm_bias[None],
        ),
        [pltpu.VMEM((mesh_rows, features), f32)],
        on_vmem=False,
    )
    return mesh_out[None, None]


def solution(mesh):
    return jax.shard_map(
        local,
        mesh=mesh,
        in_specs=(
            P("lat", "lon", None, None),
            P("lat", "lon", None, None),
            P("lat", "lon", None, None),
            P("lat", "lon", None),
            P("lat", "lon", None),
            P(),
            P(),
            P(),
            P(),
            P(),
            P(),
            P(),
            P(),
            P(),
        ),
        out_specs=P("lat", "lon", None, None),
        check_vma=False,
    )
```
